32 devices in a mesh: prow: 8 (over y, x, core), pcol: 4 (over z).
Axes of the slice: x: 2, y: 2, z: 4, core: 2. Of those that a mesh axis runs over, the one named last changes fastest.
Arguments:
- ancestor_inverse: float32 [8, 8, 512, 512], P('prow', 'pcol'), may hold values from -0.09375 to 0.09375
- factor_panel: float32 [512, 8, 3, 512], P('pcol', 'prow'), may hold values from -0.75 to 0.75
- pivot_inverse: float32 [3, 512, 512], P(None, 'prow', 'pcol'), may hold values from -6 to 6
- structure: int32 [8, 3], replicated, may hold values from 0 to 1, as said below
Outputs:
- inverse_panel: float32 [512, 8, 3, 512], P('pcol', 'prow')
- diagonal_block: float32 [3, 512, 512], P(None, 'prow', 'pcol')
The draws below stay inside these ranges and needn't reach their ends.
Inputs may be any that keep to these rules, and one draw needn't show every extreme that they name: structure[J, K] is 1 where ancestor J lies in supernode K's structure and 0 elsewhere; the last ancestor, 7, lies in every supernode's structure.
All inputs are finite; a program needn't handle non-finite values.
Results may differ from the reference program's by a relative error of at most 0.00007.
Values sent between devices are 32-bit elements; how exact they have to be, the bound alone decides.
A program may use at most 64 MiB of HBM per device.

```python
import jax
import jax.numpy as jnp
from jax import lax

B = 512
SUPER = 3
M = 8


def draw_structure(key, part):
    drawn_levels = jax.random.randint(key, (M, SUPER), 0, M)
    ancestor_index = jnp.arange(M, dtype=jnp.int32)[:, None]
    return jnp.where(drawn_levels <= ancestor_index, 1, 0).astype(jnp.int32)


def level_of(rng, extent, shards, smallest, largest):
    level = 1.0
    for position, shards_of in shards:
        draws = jax.random.uniform(jax.random.fold_in(jax.random.fold_in(rng, 6), position), (shards_of,), jnp.float32, smallest / len(shards), largest / len(shards))
        level = level * jnp.repeat(jnp.exp(draws), extent[position] // shards_of).reshape((-1,) + (1,) * (len(extent) - 1 - position))
    return level


def gaussian(rng, shape, scale, limit, pieces=(), held_as=jnp.bfloat16):
    factor_of = level_of(rng, shape, pieces, -0.22, 0.18) if pieces else 1.0
    values = jax.random.normal(rng, shape, jnp.float32) * scale * factor_of
    return jnp.minimum(jnp.maximum(values, -limit), limit).astype(held_as)


def setup_inputs(seed: int = 0) -> dict:
    keys = jax.random.split(jax.random.key(seed), 5)
    return {
        "ancestor_inverse": gaussian(keys[0], (M, M, B, B), (M * B) ** -0.5, 0.09375, ((0, 8), (1, 4)), jnp.float32),
        "factor_panel": gaussian(keys[1], (B, M, SUPER, B), 0.125, 0.75, ((0, 4), (1, 8)), jnp.float32),
        "pivot_inverse": gaussian(keys[2], (SUPER, B, B), 1.0, 6.0, ((1, 8), (2, 4)), jnp.float32),
        "structure": draw_structure(jax.random.fold_in(keys[4], 71), 0),
    }


def reference(ancestor_inverse, factor_panel, pivot_inverse, structure):
    struct_float = structure.astype(jnp.float32)
    masked = factor_panel * struct_float[None, :, :, None]

    def one_row(inverse_row):
        return jnp.einsum("Jrt,tJKc->rKc", inverse_row, masked, precision=lax.Precision.HIGHEST, preferred_element_type=jnp.float32)

    product = lax.map(one_row, ancestor_inverse)
    product = jnp.transpose(product, (1, 0, 2, 3))
    inverse_panel = -struct_float[None, :, :, None] * product
    diagonal_block = pivot_inverse - jnp.einsum("riKa,riKb->Kab", masked, inverse_panel, precision=lax.Precision.HIGHEST, preferred_element_type=jnp.float32)
    return inverse_panel, diagonal_block
```

```python
import functools

import jax
import jax.numpy as jnp
from jax import lax
from jax.experimental import pallas as pl
from jax.experimental.pallas import tpu as pltpu
from jax.sharding import PartitionSpec as P

MESH = pl.DeviceIdType.MESH
PAIR = 2


def split(value):
    high = value.astype(jnp.bfloat16)
    low = (value - high.astype(jnp.float32)).astype(jnp.bfloat16)
    return high, low


def dot3(a_high, a_low, b_high, b_low, dims):
    def one(a, b):
        return lax.dot_general(a, b, (dims, ((), ())), preferred_element_type=jnp.float32)

    return one(a_high, b_high) + (one(a_high, b_low) + one(a_low, b_high))


def kernel(
    rows_n,
    cols_n,
    struct_ref,
    factor_ref,
    inverse_ref,
    pivot_ref,
    panel_ref,
    diag_ref,
    a_full,
    a_high,
    a_low,
    staged,
    columns,
    l_high,
    l_low,
    partial,
    ring_in,
    terms,
    pair_in,
    pair_sum,
    chip_in,
    cut,
    cut_in,
    a_sem,
    hop_send,
    hop_recv,
    all_send,
    all_recv,
    ring_send,
    ring_recv,
    pair_send,
    pair_recv,
    chip_send,
    chip_recv,
    cut_send,
    cut_recv,
):
    row = lax.axis_index("prow")
    col = lax.axis_index("pcol")
    supers = factor_ref.shape[0]
    members, width = a_full.shape[0], a_full.shape[1]
    rows = factor_ref.shape[1]
    chips = rows_n // PAIR
    part = width // rows_n
    lanes = width // cols_n
    core = lax.rem(row, PAIR)
    chip = row // PAIR
    mate = chip * PAIR + (1 - core)
    group = row // members
    member = lax.rem(row, members)

    def wrap(value, size):
        return lax.rem(value + 4 * size, size)

    barrier = pltpu.get_barrier_semaphore()
    for step in range(1, rows_n):
        pl.semaphore_signal(
            barrier, inc=1, device_id={"prow": lax.rem(row + step, rows_n)}, device_id_type=MESH
        )
    for step in range(1, cols_n):
        pl.semaphore_signal(
            barrier, inc=1, device_id={"pcol": lax.rem(col + step, cols_n)}, device_id_type=MESH
        )
    pl.semaphore_wait(barrier, rows_n + cols_n - 2)

    def remote(src, dst, send, recv, where):
        return pltpu.make_async_remote_copy(
            src_ref=src, dst_ref=dst, send_sem=send, recv_sem=recv, device_id=where, device_id_type=MESH
        )

    class Hop:
        def __init__(self, src, dst, send, recv, where, stays):
            self.far = remote(src, dst, send, recv, where)
            self.near = pltpu.make_async_copy(src, dst, recv)
            self.stays = stays

        def start(self):
            pl.when(self.stays)(self.near.start)
            pl.when(jnp.logical_not(self.stays))(self.far.start)

        def wait_recv(self):
            pl.when(self.stays)(self.near.wait)
            pl.when(jnp.logical_not(self.stays))(self.far.wait_recv)

        def wait_send(self):
            pl.when(jnp.logical_not(self.stays))(self.far.wait_send)

    sent = []

    def across(k):
        to_group = lax.rem(group + col + k, cols_n)
        return Hop(
            factor_ref.at[k],
            staged.at[k],
            hop_send.at[0, k],
            hop_recv.at[0, k],
            {"prow": to_group * members + member},
            lax.rem(col + k, cols_n) == 0,
        )

    def along(k):
        to_col = wrap(group - col - k, cols_n)
        return Hop(
            staged.at[k],
            columns.at[k, member * cols_n + col],
            hop_send.at[1, k],
            hop_recv.at[1, k],
            {"pcol": to_col},
            to_col == col,
        )

    def arrived(k):
        to_col = wrap(group - col - k, cols_n)
        here = columns.at[k, slot_of(row, k)]
        return Hop(staged.at[k], here, hop_send.at[1, k], hop_recv.at[1, k], {"pcol": to_col}, to_col == col)

    def slot_of(source, k):
        return lax.rem(source, members) * cols_n + wrap(source // members - col - k, cols_n)

    def spread(k, index, source, target):
        here = columns.at[k, slot_of(source, k)]
        return remote(here, here, all_send.at[k, index], all_recv.at[k, index], {"prow": target})

    def back(source, step):
        return lax.rem(source - PAIR * step + rows_n, rows_n)

    def start_spread(k):
        arrived(k).wait_recv()
        for step in range(chips - 1, 0, -1):
            copy = spread(k, step, row, lax.rem(row + PAIR * step, rows_n))
            copy.start()
            sent.append(copy)
        copy = spread(k, 0, row, mate)
        copy.start()
        sent.append(copy)

    def forward(k):
        for step in range(1, chips):
            spread(k, step, back(row, step), mate).wait_recv()
            copy = spread(k, chips - 1 + step, back(row, step), mate)
            copy.start()
            sent.append(copy)

    def collect(k):
        spread(k, 0, mate, mate).wait_recv()
        for step in range(1, chips):
            spread(k, chips - 1 + step, back(mate, step), mate).wait_recv()

    def ring_block(step):
        return wrap(col - 1 - step, cols_n)

    def ring_copy(k, step):
        block = pl.ds(pl.multiple_of(ring_block(step) * rows, rows), rows)
        return remote(
            partial.at[k, block],
            ring_in.at[k, step],
            ring_send.at[k, step],
            ring_recv.at[k, step],
            {"pcol": lax.rem(col + 1, cols_n)},
        )

    def multiply(k, step):
        block = pl.ds(pl.multiple_of(ring_block(step) * rows, rows), rows)
        partial[k, block, :] = dot3(
            a_high[block, :], a_low[block, :], l_high[...], l_low[...], ((1,), (0,))
        )

    def start_ring(k):
        collect(k)

        def convert(index, carry):
            mask = struct_ref[col * members + index // cols_n, k].astype(jnp.float32)
            high, low = split(columns[k, index] * mask)
            at = pl.ds(pl.multiple_of(index * rows, rows), rows)
            l_high[at, :] = high
            l_low[at, :] = low
            return carry

        lax.fori_loop(0, members * cols_n, convert, 0)
        multiply(k, 0)
        copy = ring_copy(k, 0)
        copy.start()
        sent.append(copy)

        def others(step, carry):
            multiply(k, step)
            return carry

        lax.fori_loop(1, cols_n, others, 0)

    def ring_step(k, step):
        ring_copy(k, step - 1).wait_recv()
        block = pl.ds(pl.multiple_of(ring_block(step) * rows, rows), rows)
        partial[k, block, :] = partial[k, block, :] + ring_in[k, step - 1]
        copy = ring_copy(k, step)
        copy.start()
        sent.append(copy)

    def pair_copy(k):
        return remote(terms.at[k, 1 - core], pair_in.at[k], pair_send.at[k], pair_recv.at[k], {"prow": mate})

    def chip_copy(k, step):
        to_chip = lax.rem(chip + step, chips)
        return remote(
            pair_sum.at[k, to_chip],
            chip_in.at[k, step - 1],
            chip_send.at[k, step - 1],
            chip_recv.at[k, step - 1],
            {"prow": to_chip * PAIR + core},
        )

    def cut_copy(k, step):
        to_col = lax.rem(col + step, cols_n)
        return remote(
            cut.at[k, to_col],
            cut_in.at[k, step - 1],
            cut_send.at[k, step - 1],
            cut_recv.at[k, step - 1],
            {"pcol": to_col},
        )

    def finish_panel(k):
        ring_copy(k, cols_n - 2).wait_recv()
        block = pl.ds(pl.multiple_of(col * rows, rows), rows)
        mask = struct_ref[row, k].astype(jnp.float32)
        result = -mask * (partial[k, block, :] + ring_in[k, cols_n - 2])
        panel_ref[k] = result
        f_high, f_low = split(factor_ref[k] * mask)
        r_high, r_low = split(result)
        for at in range(rows_n):
            these = slice(at * part, (at + 1) * part)
            terms[k, at % PAIR, at // PAIR] = dot3(
                f_high[:, these], f_low[:, these], r_high, r_low, ((0,), (0,))
            )
        copy = pair_copy(k)
        copy.start()
        sent.append(copy)

    def add_pair(k):
        pair_copy(k).wait_recv()
        pair_sum[k] = terms[k, core] + pair_in[k]
        for step in range(chips - 1, 0, -1):
            copy = chip_copy(k, step)
            copy.start()
            sent.append(copy)

    def add_chips(k):
        total = pair_sum[k, chip]
        for step in range(1, chips):
            chip_copy(k, step).wait_recv()
            total = total + chip_in[k, step - 1]
        for at in range(cols_n):
            cut[k, at] = total[:, at * lanes : (at + 1) * lanes]
        for step in range(cols_n - 1, 0, -1):
            copy = cut_copy(k, step)
            copy.start()
            sent.append(copy)

    def add_cuts(k):
        total = cut[k, col]
        for step in range(1, cols_n):
            cut_copy(k, step).wait_recv()
            total = total + cut_in[k, step - 1]
        diag_ref[k] = pivot_ref[k] - total

    load = pltpu.make_async_copy(inverse_ref.at[0], a_full, a_sem)
    load.start()
    for k in range(supers):
        across(k).start()
        sent.append(across(k))
    for k in range(supers):
        across(k).wait_recv()
        along(k).start()
        sent.append(along(k))
    load.wait()
    for index in range(members):
        high, low = split(a_full[index])
        a_high[:, index * width : (index + 1) * width] = high
        a_low[:, index * width : (index + 1) * width] = low

    start_spread(0)
    stages = [start_ring]
    for step in range(1, cols_n - 1):
        stages.append(functools.partial(lambda at, k: ring_step(k, at), step))
    stages += [finish_panel, add_pair, add_chips, add_cuts]
    for wave in range(supers + len(stages) - 1):
        if wave < supers:
            if wave + 1 < supers:
                start_spread(wave + 1)
            forward(wave)
        for k in range(supers):
            if 0 <= wave - k < len(stages):
                stages[wave - k](k)

    for copy in sent:
        copy.wait_send()


def body(ancestor_inverse, factor_panel, pivot_inverse, structure):
    rows_n, cols_n = lax.axis_size("prow"), lax.axis_size("pcol")
    members, width = ancestor_inverse.shape[1], ancestor_inverse.shape[3]
    rows, _, supers, _ = factor_panel.shape
    chips, part, lanes = rows_n // PAIR, width // rows_n, width // cols_n
    factor = jnp.transpose(factor_panel[:, 0], (1, 0, 2))
    f32, b16, dma = jnp.float32, jnp.bfloat16, pltpu.SemaphoreType.DMA
    vmem = pl.BlockSpec(memory_space=pltpu.VMEM)
    panel, diagonal = pl.pallas_call(
        functools.partial(kernel, rows_n, cols_n),
        out_shape=(
            jax.ShapeDtypeStruct((supers, rows, width), f32),
            jax.ShapeDtypeStruct(pivot_inverse.shape, f32),
        ),
        in_specs=[
            pl.BlockSpec(memory_space=pltpu.SMEM),
            vmem,
            pl.BlockSpec(memory_space=pl.ANY),
            vmem,
        ],
        out_specs=(vmem, vmem),
        scratch_shapes=[
            pltpu.VMEM((members, width, width), f32),
            pltpu.VMEM((width, members * width), b16),
            pltpu.VMEM((width, members * width), b16),
            pltpu.VMEM((supers, rows, width), f32),
            pltpu.VMEM((supers, members * cols_n, rows, width), f32),
            pltpu.VMEM((members * width, width), b16),
            pltpu.VMEM((members * width, width), b16),
            pltpu.VMEM((supers, width, width), f32),
            pltpu.VMEM((supers, cols_n - 1, rows, width), f32),
            pltpu.VMEM((supers, PAIR, chips, part, width), f32),
            pltpu.VMEM((supers, chips, part, width), f32),
            pltpu.VMEM((supers, chips, part, width), f32),
            pltpu.VMEM((supers, chips - 1, part, width), f32),
            pltpu.VMEM((supers, cols_n, part, lanes), f32),
            pltpu.VMEM((supers, cols_n - 1, part, lanes), f32),
            dma,
            dma((2, supers)),
            dma((2, supers)),
            dma((supers, 2 * chips)),
            dma((supers, 2 * chips)),
            dma((supers, cols_n - 1)),
            dma((supers, cols_n - 1)),
            dma((supers,)),
            dma((supers,)),
            dma((supers, chips - 1)),
            dma((supers, chips - 1)),
            dma((supers, cols_n - 1)),
            dma((supers, cols_n - 1)),
        ],
        compiler_params=pltpu.CompilerParams(
            collective_id=0, has_side_effects=True, vmem_limit_bytes=56 * 1024 * 1024
        ),
    )(structure, factor, ancestor_inverse, pivot_inverse)
    return jnp.transpose(panel, (1, 0, 2))[:, None], diagonal


def solution(mesh):
    placed = (
        P("prow", "pcol", None, None),
        P("pcol", "prow", None, None),
        P(None, "prow", "pcol"),
        P(),
    )
    return jax.shard_map(
        body,
        mesh=mesh,
        in_specs=placed,
        out_specs=(P("pcol", "prow", None, None), P(None, "prow", "pcol")),
        check_vma=False,
    )
```

```python
import functools

import jax
import jax.numpy as jnp
from jax import lax
from jax.experimental import pallas as pl
from jax.experimental.pallas import tpu as pltpu
from jax.sharding import PartitionSpec as P

MESH = pl.DeviceIdType.MESH
PAIR = 2
HALVES = 2


def split(value):
    high = value.astype(jnp.bfloat16)
    low = (value - high.astype(jnp.float32)).astype(jnp.bfloat16)
    return high, low


def dot3(a_high, a_low, b_high, b_low, dims):
    def one(a, b):
        return lax.dot_general(a, b, (dims, ((), ())), preferred_element_type=jnp.float32)

    return one(a_high, b_high) + (one(a_high, b_low) + one(a_low, b_high))


def kernel(
    rows_n,
    cols_n,
    struct_ref,
    factor_ref,
    inverse_ref,
    pivot_ref,
    panel_ref,
    diag_ref,
    a_full,
    a_high,
    a_low,
    staged,
    columns,
    l_high,
    l_low,
    partial,
    ring_in,
    terms,
    pair_in,
    pair_sum,
    chip_in,
    cut,
    cut_in,
    a_sem,
    hop_send,
    hop_recv,
    all_send,
    all_recv,
    ring_send,
    ring_recv,
    pair_send,
    pair_recv,
    chip_send,
    chip_recv,
    cut_send,
    cut_recv,
):
    row = lax.axis_index("prow")
    col = lax.axis_index("pcol")
    chunks = factor_ref.shape[0]
    supers = chunks // HALVES
    members, width = a_full.shape[0], a_full.shape[1]
    rows = factor_ref.shape[1]
    chips = rows_n // PAIR
    part = width // rows_n
    lanes = width // cols_n
    core = lax.rem(row, PAIR)
    chip = row // PAIR
    mate = chip * PAIR + (1 - core)
    group = row // members
    member = lax.rem(row, members)

    def wrap(value, size):
        return lax.rem(value + 4 * size, size)

    barrier = pltpu.get_barrier_semaphore()
    for step in range(1, rows_n):
        pl.semaphore_signal(
            barrier, inc=1, device_id={"prow": lax.rem(row + step, rows_n)}, device_id_type=MESH
        )
    for step in range(1, cols_n):
        pl.semaphore_signal(
            barrier, inc=1, device_id={"pcol": lax.rem(col + step, cols_n)}, device_id_type=MESH
        )
    pl.semaphore_wait(barrier, rows_n + cols_n - 2)

    def remote(src, dst, send, recv, where):
        return pltpu.make_async_remote_copy(
            src_ref=src, dst_ref=dst, send_sem=send, recv_sem=recv, device_id=where, device_id_type=MESH
        )

    class Hop:
        def __init__(self, src, dst, send, recv, where, stays):
            self.far = remote(src, dst, send, recv, where)
            self.near = pltpu.make_async_copy(src, dst, recv)
            self.stays = stays

        def start(self):
            pl.when(self.stays)(self.near.start)
            pl.when(jnp.logical_not(self.stays))(self.far.start)

        def wait_recv(self):
            pl.when(self.stays)(self.near.wait)
            pl.when(jnp.logical_not(self.stays))(self.far.wait_recv)

        def wait_send(self):
            pl.when(jnp.logical_not(self.stays))(self.far.wait_send)

    sent = []

    def across(k):
        to_group = lax.rem(group + col + k, cols_n)
        return Hop(
            factor_ref.at[k],
            staged.at[k],
            hop_send.at[0, k],
            hop_recv.at[0, k],
            {"prow": to_group * members + member},
            lax.rem(col + k, cols_n) == 0,
        )

    def along(k):
        to_col = wrap(group - col - k, cols_n)
        return Hop(
            staged.at[k],
            columns.at[k, member * cols_n + col],
            hop_send.at[1, k],
            hop_recv.at[1, k],
            {"pcol": to_col},
            to_col == col,
        )

    def arrived(k):
        to_col = wrap(group - col - k, cols_n)
        here = columns.at[k, slot_of(row, k)]
        return Hop(staged.at[k], here, hop_send.at[1, k], hop_recv.at[1, k], {"pcol": to_col}, to_col == col)

    def slot_of(source, k):
        return lax.rem(source, members) * cols_n + wrap(source // members - col - k, cols_n)

    def spread(k, index, source, target):
        here = columns.at[k, slot_of(source, k)]
        return remote(here, here, all_send.at[k, index], all_recv.at[k, index], {"prow": target})

    def back(source, step):
        return lax.rem(source - PAIR * step + rows_n, rows_n)

    def start_spread(k):
        arrived(k).wait_recv()
        for step in range(chips - 1, 0, -1):
            copy = spread(k, step, row, lax.rem(row + PAIR * step, rows_n))
            copy.start()
            sent.append(copy)
        copy = spread(k, 0, row, mate)
        copy.start()
        sent.append(copy)

    def forward(k):
        for step in range(1, chips):
            spread(k, step, back(row, step), mate).wait_recv()
            copy = spread(k, chips - 1 + step, back(row, step), mate)
            copy.start()
            sent.append(copy)

    def collect(k):
        spread(k, 0, mate, mate).wait_recv()
        for step in range(1, chips):
            spread(k, chips - 1 + step, back(mate, step), mate).wait_recv()

    def ring_block(step):
        return wrap(col - 1 - step, cols_n)

    def ring_copy(k, step):
        block = pl.ds(pl.multiple_of(ring_block(step) * rows, rows), rows)
        return remote(
            partial.at[k, block],
            ring_in.at[k, step],
            ring_send.at[k, step],
            ring_recv.at[k, step],
            {"pcol": lax.rem(col + 1, cols_n)},
        )

    def multiply(k, step):
        block = pl.ds(pl.multiple_of(ring_block(step) * rows, rows), rows)
        partial[k, block, :] = dot3(
            a_high[block, :], a_low[block, :], l_high[...], l_low[...], ((1,), (0,))
        )

    def start_ring(k):
        collect(k)

        def convert(index, carry):
            mask = struct_ref[col * members + index // cols_n, k // HALVES].astype(jnp.float32)
            high, low = split(columns[k, index] * mask)
            at = pl.ds(pl.multiple_of(index * rows, rows), rows)
            l_high[at, :] = high
            l_low[at, :] = low
            return carry

        lax.fori_loop(0, members * cols_n, convert, 0)
        multiply(k, 0)
        copy = ring_copy(k, 0)
        copy.start()
        sent.append(copy)

        def others(step, carry):
            multiply(k, step)
            return carry

        lax.fori_loop(1, cols_n, others, 0)

    def ring_step(k, step):
        ring_copy(k, step - 1).wait_recv()
        block = pl.ds(pl.multiple_of(ring_block(step) * rows, rows), rows)
        partial[k, block, :] = partial[k, block, :] + ring_in[k, step - 1]
        copy = ring_copy(k, step)
        copy.start()
        sent.append(copy)

    def pair_copy(k):
        return remote(terms.at[k, 1 - core], pair_in.at[k], pair_send.at[k], pair_recv.at[k], {"prow": mate})

    def chip_copy(k, step):
        to_chip = lax.rem(chip + step, chips)
        return remote(
            pair_sum.at[k, to_chip],
            chip_in.at[k, step - 1],
            chip_send.at[k, step - 1],
            chip_recv.at[k, step - 1],
            {"prow": to_chip * PAIR + core},
        )

    def cut_copy(k, step):
        to_col = lax.rem(col + step, cols_n)
        return remote(
            cut.at[k, to_col],
            cut_in.at[k, step - 1],
            cut_send.at[k, step - 1],
            cut_recv.at[k, step - 1],
            {"pcol": to_col},
        )

    def finish_panel(k):
        ring_copy(k, cols_n - 2).wait_recv()
        block = pl.ds(pl.multiple_of(col * rows, rows), rows)
        mask = struct_ref[row, k // HALVES].astype(jnp.float32)
        result = -mask * (partial[k, block, :] + ring_in[k, cols_n - 2])
        panel_ref[k] = result
        r_high, r_low = split(result)
        for half in range(HALVES):
            f_high, f_low = split(factor_ref[k // HALVES * HALVES + half] * mask)
            term = dot3(f_high, f_low, r_high, r_low, ((0,), (0,)))
            for here in range(rows_n // HALVES):
                at = half * (rows_n // HALVES) + here
                terms[k, at % PAIR, at // PAIR] = term[here * part : (here + 1) * part]
        copy = pair_copy(k)
        copy.start()
        sent.append(copy)

    def add_pair(k):
        pair_copy(k).wait_recv()
        pair_sum[k] = terms[k, core] + pair_in[k]
        for step in range(chips - 1, 0, -1):
            copy = chip_copy(k, step)
            copy.start()
            sent.append(copy)

    def add_chips(k):
        total = pair_sum[k, chip]
        for step in range(1, chips):
            chip_copy(k, step).wait_recv()
            total = total + chip_in[k, step - 1]
        for at in range(cols_n // HALVES):
            cut[k // HALVES, k % HALVES * (cols_n // HALVES) + at] = total[:, at * lanes : (at + 1) * lanes]
        if k % HALVES == HALVES - 1:
            for step in range(cols_n - 1, 0, -1):
                copy = cut_copy(k // HALVES, step)
                copy.start()
                sent.append(copy)

    def add_cuts(k):
        if k % HALVES < HALVES - 1:
            return
        at = k // HALVES
        total = cut[at, col]
        for step in range(1, cols_n):
            cut_copy(at, step).wait_recv()
            total = total + cut_in[at, step - 1]
        diag_ref[at] = pivot_ref[at] - total

    load = pltpu.make_async_copy(inverse_ref.at[0], a_full, a_sem)
    load.start()
    for k in range(chunks):
        across(k).start()
        sent.append(across(k))
    for k in range(chunks):
        across(k).wait_recv()
        along(k).start()
        sent.append(along(k))
    load.wait()
    for index in range(members):
        high, low = split(a_full[index])
        a_high[:, index * width : (index + 1) * width] = high
        a_low[:, index * width : (index + 1) * width] = low

    start_spread(0)
    stages = [start_ring]
    for step in range(1, cols_n - 1):
        stages.append(functools.partial(lambda at, k: ring_step(k, at), step))
    stages += [finish_panel, add_pair, add_chips, add_cuts]
    for wave in range(chunks + len(stages) - 1):
        if wave < chunks:
            if wave + 1 < chunks:
                start_spread(wave + 1)
            forward(wave)
        for k in range(chunks):
            if 0 <= wave - k < len(stages):
                stages[wave - k](k)

    for copy in sent:
        copy.wait_send()


def body(ancestor_inverse, factor_panel, pivot_inverse, structure):
    rows_n, cols_n = lax.axis_size("prow"), lax.axis_size("pcol")
    members, width = ancestor_inverse.shape[1], ancestor_inverse.shape[3]
    rows, _, supers, _ = factor_panel.shape
    chips, part, lanes = rows_n // PAIR, width // rows_n, width // cols_n
    chunks, piece = supers * HALVES, width // HALVES
    factor = jnp.transpose(factor_panel.reshape(rows, chunks, piece), (1, 0, 2))
    f32, b16, dma = jnp.float32, jnp.bfloat16, pltpu.SemaphoreType.DMA
    vmem = pl.BlockSpec(memory_space=pltpu.VMEM)
    panel, diagonal = pl.pallas_call(
        functools.partial(kernel, rows_n, cols_n),
        out_shape=(
            jax.ShapeDtypeStruct((chunks, rows, piece), f32),
            jax.ShapeDtypeStruct(pivot_inverse.shape, f32),
        ),
        in_specs=[
            pl.BlockSpec(memory_space=pltpu.SMEM),
            vmem,
            pl.BlockSpec(memory_space=pl.ANY),
            vmem,
        ],
        out_specs=(vmem, vmem),
        scratch_shapes=[
            pltpu.VMEM((members, width, width), f32),
            pltpu.VMEM((width, members * width), b16),
            pltpu.VMEM((width, members * width), b16),
            pltpu.VMEM((chunks, rows, piece), f32),
            pltpu.VMEM((chunks, members * cols_n, rows, piece), f32),
            pltpu.VMEM((members * width, piece), b16),
            pltpu.VMEM((members * width, piece), b16),
            pltpu.VMEM((chunks, width, piece), f32),
            pltpu.VMEM((chunks, cols_n - 1, rows, piece), f32),
            pltpu.VMEM((chunks, PAIR, chips, part, piece), f32),
            pltpu.VMEM((chunks, chips, part, piece), f32),
            pltpu.VMEM((chunks, chips, part, piece), f32),
            pltpu.VMEM((chunks, chips - 1, part, piece), f32),
            pltpu.VMEM((supers, cols_n, part, lanes), f32),
            pltpu.VMEM((supers, cols_n - 1, part, lanes), f32),
            dma,
            dma((2, chunks)),
            dma((2, chunks)),
            dma((chunks, 2 * chips)),
            dma((chunks, 2 * chips)),
            dma((chunks, cols_n - 1)),
            dma((chunks, cols_n - 1)),
            dma((chunks,)),
            dma((chunks,)),
            dma((chunks, chips - 1)),
            dma((chunks, chips - 1)),
            dma((supers, cols_n - 1)),
            dma((supers, cols_n - 1)),
        ],
        compiler_params=pltpu.CompilerParams(
            collective_id=0, has_side_effects=True, vmem_limit_bytes=56 * 1024 * 1024
        ),
    )(structure, factor, ancestor_inverse, pivot_inverse)
    return jnp.transpose(panel, (1, 0, 2)).reshape(factor_panel.shape), diagonal


def solution(mesh):
    placed = (
        P("prow", "pcol", None, None),
        P("pcol", "prow", None, None),
        P(None, "prow", "pcol"),
        P(),
    )
    return jax.shard_map(
        body,
        mesh=mesh,
        in_specs=placed,
        out_specs=(P("pcol", "prow", None, None), P(None, "prow", "pcol")),
        check_vma=False,
    )
```
